64 devices in a mesh: dp: 4 (over x, y), tp: 16 (over z, core).
Axes of the slice: x: 2, y: 2, z: 8, core: 2. Of those that a mesh axis runs over, the one named last changes fastest.
The devices are a block of a 4x4x8 slice.
Arguments:
- x_norm: bfloat16 [32768, 2048], P(('dp', 'tp')), parts along dimension 0
- grad_out: bfloat16 [32768, 2048], P(('dp', 'tp')), parts along dimension 0
- w_gate: bfloat16 [2048, 5632], P(None, 'tp')
- w_up: bfloat16 [2048, 5632], P(None, 'tp')
- w_down: bfloat16 [5632, 2048], P('tp')
Outputs:
- output 1: bfloat16 [32768, 2048], P(('dp', 'tp')), parts along dimension 0
- output 2: float32 [8192, 5632], P('dp', 'tp'), parts along dimension 0
- output 3: float32 [8192, 5632], P('dp', 'tp'), parts along dimension 0
- output 4: float32 [22528, 2048], P(('dp', 'tp')), parts along dimension 0
There are 4 independent parts. The reference program is written for one: setup_inputs(seed, part) draws one part's arguments, and reference() takes and returns one part's arrays. A program takes and returns all parts, laid end to end along the dimension named above; an argument that names none is the same for every part.
All inputs are finite; a program needn't handle non-finite values.
Results may differ from the reference program's by a relative error of at most 0.0166201.
Values are sent between devices in bfloat16 or wider.
A program may use at most 768 MiB of HBM per device.

```python
import jax
import jax.numpy as jnp
from jax import lax

TOKENS = 8192
HIDDEN = 2048
FFN_DIM = 5632


def setup_inputs(seed: int = 0, part: int = 0) -> dict:
    key = jax.random.key(seed)
    key_gate, key_up, key_down, key_act = jax.random.split(key, 4)
    key_part = jax.random.fold_in(key_act, part)
    key_x, key_dy = jax.random.split(key_part)
    x_norm = jax.random.normal(key_x, (TOKENS, HIDDEN), jnp.float32).astype(jnp.bfloat16)
    grad_out = jax.random.normal(key_dy, (TOKENS, HIDDEN), jnp.float32).astype(jnp.bfloat16)
    w_gate = (jax.random.normal(key_gate, (HIDDEN, FFN_DIM), jnp.float32) * HIDDEN ** -0.5).astype(jnp.bfloat16)
    w_up = (jax.random.normal(key_up, (HIDDEN, FFN_DIM), jnp.float32) * HIDDEN ** -0.5).astype(jnp.bfloat16)
    w_down = (jax.random.normal(key_down, (FFN_DIM, HIDDEN), jnp.float32) * FFN_DIM ** -0.5).astype(jnp.bfloat16)
    return {"x_norm": x_norm, "grad_out": grad_out, "w_gate": w_gate, "w_up": w_up, "w_down": w_down}


def reference(x_norm, grad_out, w_gate, w_up, w_down):
    contract_rows = (((0,), (0,)), ((), ()))
    contract_cols = (((1,), (1,)), ((), ()))
    gate_pre = jnp.dot(x_norm, w_gate, preferred_element_type=jnp.float32).astype(jnp.bfloat16).astype(jnp.float32)
    up_pre = jnp.dot(x_norm, w_up, preferred_element_type=jnp.float32).astype(jnp.bfloat16).astype(jnp.float32)
    gate_sig = jax.nn.sigmoid(gate_pre)
    gate_act = gate_pre * gate_sig
    mid_act = (gate_act * up_pre).astype(jnp.bfloat16)
    grad_w_down = lax.dot_general(mid_act, grad_out, contract_rows, preferred_element_type=jnp.float32)
    grad_mid = lax.dot_general(grad_out, w_down, contract_cols, preferred_element_type=jnp.float32)
    grad_up = (grad_mid * gate_act).astype(jnp.bfloat16)
    grad_gate = (grad_mid * up_pre * gate_sig * (1.0 + gate_pre * (1.0 - gate_sig))).astype(jnp.bfloat16)
    grad_x = (lax.dot_general(grad_gate, w_gate, contract_cols, preferred_element_type=jnp.float32)
              + lax.dot_general(grad_up, w_up, contract_cols, preferred_element_type=jnp.float32)).astype(jnp.bfloat16)
    grad_w_gate = lax.dot_general(x_norm, grad_gate, contract_rows, preferred_element_type=jnp.float32)
    grad_w_up = lax.dot_general(x_norm, grad_up, contract_rows, preferred_element_type=jnp.float32)
    return (grad_x, grad_w_gate, grad_w_up, grad_w_down)
```

```python
import jax
import jax.numpy as jnp
from jax import lax
from jax.experimental import pallas as pl
from jax.experimental.pallas import tpu as pltpu
from jax.sharding import PartitionSpec as P


F32, BF16 = jnp.float32, jnp.bfloat16
BLOCK = 512
LANES = 128


def token_kernel(has_received, x_ref, dy_ref, w_in_ref, w_down_ref, w_back_ref, *refs):
    received_ref, (mid_ref, grad_ref, part_ref) = (refs[0], refs[1:]) if has_received else (None, refs)
    width = mid_ref.shape[1]
    pre = jnp.dot(x_ref[...], w_in_ref[...], preferred_element_type=F32).astype(BF16).astype(F32)
    gate, up = pre[:, :width], pre[:, width:]
    grad_mid = jnp.dot(dy_ref[...], w_down_ref[...], preferred_element_type=F32)
    sig = jax.nn.sigmoid(gate)
    act = gate * sig
    mid_ref[...] = (act * up).astype(BF16)
    grad_ref[:, :width] = (grad_mid * up * sig * (1.0 + gate * (1.0 - sig))).astype(BF16)
    grad_ref[:, width:] = (grad_mid * act).astype(BF16)
    part = jnp.dot(grad_ref[...], w_back_ref[...], preferred_element_type=F32)
    if has_received:
        part = part + received_ref[...].astype(F32)
    part_ref[...] = part.astype(BF16)


def token_call(x, dy, w_in, w_down, w_back, received=None):
    rows, hidden = x.shape
    width = w_down.shape[1]
    block = min(BLOCK, rows)
    tokens = lambda n: pl.BlockSpec((block, n), lambda i: (i, 0))
    whole = lambda a: pl.BlockSpec(a.shape, lambda i: (0, 0))
    args = [x, dy, w_in, w_down, w_back] + ([] if received is None else [received])
    specs = [tokens(hidden), tokens(hidden), whole(w_in), whole(w_down), whole(w_back)]
    specs += [] if received is None else [tokens(hidden)]
    return pl.pallas_call(
        lambda *refs: token_kernel(received is not None, *refs),
        grid=(rows // block,),
        in_specs=specs,
        out_specs=[tokens(width), tokens(2 * width), tokens(hidden)],
        out_shape=[jax.ShapeDtypeStruct((rows, n), BF16) for n in (width, 2 * width, hidden)],
        compiler_params=pltpu.CompilerParams(dimension_semantics=("arbitrary",), vmem_limit_bytes=60 * 2**20),
        cost_estimate=pl.CostEstimate(flops=10 * rows * hidden * width, bytes_accessed=8 * rows * hidden,
                                      transcendentals=rows * width),
        name="token_part",
    )(*args)


def weight_kernel(has_acc, x_ref, dy_ref, mid_ref, grad_ref, *refs):
    acc_refs, outs = (refs[:3], refs[3:]) if has_acc else ((), refs)
    inner, width = outs[0].shape[0], mid_ref.shape[1]

    @pl.when(pl.program_id(0) == 0)
    def _():
        if has_acc:
            for acc, out in zip(acc_refs, outs):
                pltpu.sync_copy(acc, out)
        else:
            for out in outs:
                out[...] = jnp.zeros_like(out)

    rows_by_rows = (((0,), (0,)), ((), ()))
    for out, left, right in ((outs[0], grad_ref[:, :width], x_ref), (outs[1], grad_ref[:, width:], x_ref),
                             (outs[2], mid_ref[...], dy_ref)):
        term = lax.dot_general(left, right[...], rows_by_rows, preferred_element_type=F32)
        out[...] += term[:inner]


def weight_call(x, dy, mid, grad, inner, acc):
    rows, hidden = x.shape
    width = mid.shape[1]
    block = min(BLOCK, rows)
    tokens = lambda n: pl.BlockSpec((block, n), lambda i: (i, 0))
    return pl.pallas_call(
        lambda *refs: weight_kernel(acc is not None, *refs),
        grid=(rows // block,),
        in_specs=[tokens(hidden), tokens(hidden), tokens(width), tokens(2 * width)]
        + ([] if acc is None else [pl.BlockSpec(memory_space=pl.ANY)] * 3),
        out_specs=[pl.BlockSpec((inner, hidden), lambda i: (0, 0))] * 3,
        out_shape=[jax.ShapeDtypeStruct((inner, hidden), F32)] * 3,
        compiler_params=pltpu.CompilerParams(dimension_semantics=("arbitrary",), vmem_limit_bytes=60 * 2**20),
        cost_estimate=pl.CostEstimate(flops=6 * rows * hidden * width,
                                      bytes_accessed=4 * rows * hidden + 24 * inner * hidden, transcendentals=0),
        name="weight_part",
    )(x, dy, mid, grad, *(() if acc is None else acc))


def after(value, *earlier):
    return lax.optimization_barrier((value, *earlier))[0]


def solution(mesh):
    tp = mesh.shape["tp"]
    rings = [list(range(core, tp, 2)) for core in range(2)]
    swap = [(i, i ^ 1) for i in range(tp)]

    def gather(shard):
        return lax.all_gather(shard, "tp", axis=0, tiled=True, axis_index_groups=rings)

    def scatter(part):
        return lax.psum_scatter(part, "tp", scatter_dimension=0, tiled=True, axis_index_groups=rings)

    def swapped(value):
        return lax.ppermute(value, "tp", swap)

    def device_step(x_shard, dy_shard, w_gate, w_up, w_down):
        rows, inner = x_shard.shape[0], w_down.shape[0]
        cut = rows * 5 // 8
        pad = -inner % LANES
        w_in = jnp.concatenate([jnp.pad(w, ((0, 0), (0, pad))) for w in (w_gate, w_up)], axis=1)
        w_back = jnp.concatenate([jnp.pad(w.T, ((0, pad), (0, 0))) for w in (w_gate, w_up)], axis=0)
        w_mid = jnp.pad(w_down.T, ((0, 0), (0, pad)))
        weights = (w_in, w_mid, w_back)

        x0 = gather(x_shard[:cut])
        dy0 = gather(dy_shard[:cut])
        x1 = gather(x_shard[cut:])
        dy1 = gather(dy_shard[cut:])
        x0_other, dy0_other, x1_other, dy1_other = (swapped(a) for a in (x0, dy0, x1, dy1))

        *rest0_other, part0_other = token_call(x0_other, dy0_other, *weights)
        *rest0, part0 = token_call(x0, dy0, *weights, swapped(part0_other))
        sum0 = scatter(part0)
        acc = weight_call(x0_other, after(dy0_other, part0), *rest0_other, inner, None)

        *rest1_other, part1_other = token_call(x1_other, dy1_other, after(w_in, acc[0]), w_mid, w_back)
        *rest1, part1 = token_call(x1, dy1, *weights, swapped(part1_other))
        sum1 = scatter(part1)
        acc = weight_call(x0, after(dy0, part1), *rest0, inner, acc)
        acc = weight_call(x1_other, dy1_other, *rest1_other, inner, acc)
        acc = weight_call(x1, dy1, *rest1, inner, acc)
        return jnp.concatenate([sum0, sum1], axis=0), acc[0].T, acc[1].T, acc[2]

    tok_spec = P(("dp", "tp"), None)
    col_spec = P(None, "tp")
    grad_col_spec = P("dp", "tp")
    return jax.shard_map(device_step, mesh=mesh,
                         in_specs=(tok_spec, tok_spec, col_spec, col_spec, P("tp", None)),
                         out_specs=(tok_spec, grad_col_spec, grad_col_spec, tok_spec),
                         check_vma=False)
```

```python
import jax
import jax.numpy as jnp
from jax import lax
from jax.experimental import pallas as pl
from jax.experimental.pallas import tpu as pltpu
from jax.sharding import PartitionSpec as P


F32, BF16 = jnp.float32, jnp.bfloat16
SHARDS = 2
LANES = 128


def flat(ref):
    return ref[...].reshape(-1, ref.shape[-1])


def token_kernel(has_received, x_ref, dy_ref, w_in_ref, w_down_ref, w_back_ref, *refs):
    received_ref, (mid_ref, grad_ref, part_ref) = (refs[0], refs[1:]) if has_received else (None, refs)
    width = mid_ref.shape[1]
    pre = jnp.dot(flat(x_ref), w_in_ref[...], preferred_element_type=F32).astype(BF16).astype(F32)
    gate, up = pre[:, :width], pre[:, width:]
    grad_mid = jnp.dot(flat(dy_ref), w_down_ref[...], preferred_element_type=F32)
    sig = jax.nn.sigmoid(gate)
    act = gate * sig
    mid_ref[...] = (act * up).astype(BF16)
    grad_ref[:, :width] = (grad_mid * up * sig * (1.0 + gate * (1.0 - sig))).astype(BF16)
    grad_ref[:, width:] = (grad_mid * act).astype(BF16)
    part = jnp.dot(grad_ref[...], w_back_ref[...], preferred_element_type=F32)
    if has_received:
        part = part + received_ref[...].astype(F32)
    part_ref[...] = part.astype(BF16)


def halves(both):
    _, _, rows, hidden = both.shape
    return [pl.BlockSpec((SHARDS, None, rows, hidden), lambda i, part=part: (i, part, 0, 0)) for part in range(2)]


def token_call(both, w_in, w_down, w_back, received=None):
    shards, _, shard_rows, hidden = both.shape
    rows, block = shards * shard_rows, SHARDS * shard_rows
    width = w_down.shape[1]
    tokens = lambda n: pl.BlockSpec((block, n), lambda i: (i, 0))
    whole = lambda a: pl.BlockSpec(a.shape, lambda i: (0, 0))
    args = [both, both, w_in, w_down, w_back] + ([] if received is None else [received])
    specs = halves(both) + [whole(w_in), whole(w_down), whole(w_back)]
    specs += [] if received is None else [tokens(hidden)]
    return pl.pallas_call(
        lambda *refs: token_kernel(received is not None, *refs),
        grid=(shards // SHARDS,),
        in_specs=specs,
        out_specs=[tokens(width), tokens(2 * width), tokens(hidden)],
        out_shape=[jax.ShapeDtypeStruct((rows, n), BF16) for n in (width, 2 * width, hidden)],
        compiler_params=pltpu.CompilerParams(dimension_semantics=("arbitrary",), vmem_limit_bytes=60 * 2**20),
        cost_estimate=pl.CostEstimate(flops=10 * rows * hidden * width, bytes_accessed=8 * rows * hidden,
                                      transcendentals=rows * width),
        name="token_part",
    )(*args)


def weight_kernel(has_acc, x_ref, dy_ref, mid_ref, grad_ref, *refs):
    acc_refs, outs = (refs[:3], refs[3:]) if has_acc else ((), refs)
    inner, width = outs[0].shape[0], mid_ref.shape[1]

    @pl.when(pl.program_id(0) == 0)
    def _():
        if has_acc:
            for acc, out in zip(acc_refs, outs):
                pltpu.sync_copy(acc, out)
        else:
            for out in outs:
                out[...] = jnp.zeros_like(out)

    rows_by_rows = (((0,), (0,)), ((), ()))
    for out, left, right in ((outs[0], grad_ref[:, :width], x_ref), (outs[1], grad_ref[:, width:], x_ref),
                             (outs[2], mid_ref[...], dy_ref)):
        term = lax.dot_general(left, flat(right), rows_by_rows, preferred_element_type=F32)
        out[...] += term[:inner]


def weight_call(both, mid, grad, inner, acc):
    shards, _, shard_rows, hidden = both.shape
    rows, block = shards * shard_rows, SHARDS * shard_rows
    width = mid.shape[1]
    tokens = lambda n: pl.BlockSpec((block, n), lambda i: (i, 0))
    return pl.pallas_call(
        lambda *refs: weight_kernel(acc is not None, *refs),
        grid=(shards // SHARDS,),
        in_specs=halves(both) + [tokens(width), tokens(2 * width)]
        + ([] if acc is None else [pl.BlockSpec(memory_space=pl.ANY)] * 3),
        out_specs=[pl.BlockSpec((inner, hidden), lambda i: (0, 0))] * 3,
        out_shape=[jax.ShapeDtypeStruct((inner, hidden), F32)] * 3,
        compiler_params=pltpu.CompilerParams(dimension_semantics=("arbitrary",), vmem_limit_bytes=60 * 2**20),
        cost_estimate=pl.CostEstimate(flops=6 * rows * hidden * width,
                                      bytes_accessed=4 * rows * hidden + 24 * inner * hidden, transcendentals=0),
        name="weight_part",
    )(both, both, mid, grad, *(() if acc is None else acc))


def after(value, *earlier):
    return lax.optimization_barrier((value, *earlier))[0]


def solution(mesh):
    tp = mesh.shape["tp"]
    rings = [list(range(core, tp, 2)) for core in range(2)]
    swap = [(i, i ^ 1) for i in range(tp)]

    def gather(x, dy):
        both = lax.all_gather(jnp.concatenate([x, dy], axis=0), "tp", axis=0, tiled=True, axis_index_groups=rings)
        return both.reshape(-1, 2, *x.shape)

    def scatter(part):
        return lax.psum_scatter(part, "tp", scatter_dimension=0, tiled=True, axis_index_groups=rings)

    def swapped(value):
        return lax.ppermute(value, "tp", swap)

    def device_step(x_shard, dy_shard, w_gate, w_up, w_down):
        rows, inner = x_shard.shape[0], w_down.shape[0]
        cut = rows * 5 // 8
        pad = -inner % LANES
        w_in = jnp.concatenate([jnp.pad(w, ((0, 0), (0, pad))) for w in (w_gate, w_up)], axis=1)
        w_back = jnp.concatenate([jnp.pad(w.T, ((0, pad), (0, 0))) for w in (w_gate, w_up)], axis=0)
        w_mid = jnp.pad(w_down.T, ((0, 0), (0, pad)))
        weights = (w_in, w_mid, w_back)

        both0 = gather(x_shard[:cut], dy_shard[:cut])
        both1 = gather(x_shard[cut:], dy_shard[cut:])
        both0_other, both1_other = swapped(both0), swapped(both1)

        *rest0_other, part0_other = token_call(both0_other, *weights)
        *rest0, part0 = token_call(both0, *weights, swapped(part0_other))
        sum0 = scatter(part0)
        acc = weight_call(both0_other, *after(rest0_other, part0), inner, None)

        *rest1_other, part1_other = token_call(both1_other, after(w_in, acc[0]), w_mid, w_back)
        *rest1, part1 = token_call(both1, *weights, swapped(part1_other))
        sum1 = scatter(part1)
        acc = weight_call(both0, *after(rest0, part1), inner, acc)
        acc = weight_call(both1_other, *rest1_other, inner, acc)
        acc = weight_call(both1, *rest1, inner, acc)
        grad_x = lax.dynamic_update_slice(after(jnp.pad(sum0, ((0, rows - cut), (0, 0)))), sum1, (cut, 0))
        return grad_x, acc[0].T, acc[1].T, acc[2]

    tok_spec = P(("dp", "tp"), None)
    col_spec = P(None, "tp")
    grad_col_spec = P("dp", "tp")
    return jax.shard_map(device_step, mesh=mesh,
                         in_specs=(tok_spec, tok_spec, col_spec, col_spec, P("tp", None)),
                         out_specs=(tok_spec, grad_col_spec, grad_col_spec, tok_spec),
                         check_vma=False)
```
